32 devices in a mesh: groups: 2 (over x), patch: 16 (over z, y, core).
Axes of the slice: x: 2, y: 2, z: 4, core: 2. Of those that a mesh axis runs over, the one named last changes fastest.
Arguments:
- grid_latents: bfloat16 [32768, 512], P(('groups', 'patch')), parts along dimension 0, may hold values from -6 to 6
- mesh_latents: bfloat16 [16384, 512], P(('groups', 'patch')), parts along dimension 0, may hold values from -6 to 6
- enc_send: int32 [640, 128], P(('groups', 'patch')), parts along dimension 0, may hold values from 0 to 1023
- enc_recv: int32 [640, 128], P(('groups', 'patch')), parts along dimension 0, may hold values from 0 to 512, as said below
- neighbours: int32 [16384, 32], P(('groups', 'patch')), parts along dimension 0, may hold values from 0 to 8191, as said below
- enc_grid_w: bfloat16 [512, 512], replicated, may hold values from -0.25 to 0.25
- enc_bias: float32 [512], replicated, may hold values from -4 to 4
- enc_mesh_w: bfloat16 [512, 512], replicated, may hold values from -0.25 to 0.25
- enc_msg_w: bfloat16 [512, 512], replicated, may hold values from -0.25 to 0.25
- upd_agg_w: bfloat16 [512, 512], replicated, may hold values from -0.25 to 0.25
- upd_mesh_w: bfloat16 [512, 512], replicated, may hold values from -0.25 to 0.25
- upd_out_w: bfloat16 [512, 512], replicated, may hold values from -0.25 to 0.25
- norm_gain: float32 [512], replicated, may hold values from 0.1 to 1.9
- query_w: bfloat16 [512, 512], replicated, may hold values from -0.25 to 0.25
- key_w: bfloat16 [512, 512], replicated, may hold values from -0.25 to 0.25
- value_w: bfloat16 [512, 512], replicated, may hold values from -0.25 to 0.25
- out_w: bfloat16 [512, 512], replicated, may hold values from -0.25 to 0.25
- ffn_gain: float32 [512], replicated, may hold values from 0.1 to 1.9
- ffn_in_w: bfloat16 [512, 2048], replicated, may hold values from -0.25 to 0.25
- ffn_out_w: bfloat16 [2048, 512], replicated, may hold values from -0.125 to 0.125
Outputs:
- result: bfloat16 [16384, 512], P(('groups', 'patch')), parts along dimension 0
The draws below stay inside these ranges and needn't reach their ends.
There are 2 independent parts, one for each index of `groups`. The reference program is written for one: setup_inputs(seed, part) draws one part's arguments, and reference() takes and returns one part's arrays. A program takes and returns all parts, laid end to end along the dimension named above; an argument that names none is the same for every part. Nothing has to cross between parts.
Inputs may be any that keep to these rules, and one draw needn't show every extreme that they name: `enc_recv`: in each band's slots for one owner, the used edges come first and the rest hold 512; the first and last bands fill all their slots. `neighbours`: neighbour 0 of a node is the node itself; every neighbour's owner is within 2 patch indices of the node's owner, wrapping around.
All inputs are finite; a program needn't handle non-finite values.
Results may differ from the reference program's by a relative error of at most 0.006.
The reference program's roundings to bfloat16 on the way count: a program that leaves them out, or rounds other values in their place, can miss the bound.
Values may be sent and summed in bfloat16 or wider, within the bound.
No kernel may reach another device: no remote copies, remote signals or barrier semaphores. Data moves between devices by JAX's collectives and lax.ppermute only.
A program may use at most 256 MiB of HBM per device.

```python
import math
import jax
import jax.numpy as jnp
from jax import lax

D = 512
HEADS = 4
FF = 2048
G_DEV = 1024
M_DEV = 512
EB = 4
EDGE_BLOCK = 128
REACH = 2
KNB = 32
GRID = 16384
MESH = 8192
BLOCKS = 320
N_PATCH = 16


def draw_enc_recv(key, part):
    capacity = EB * EDGE_BLOCK
    hop_count = 2 * REACH + 1
    devices = jnp.arange(N_PATCH, dtype=jnp.int32)
    distance = jnp.abs(2 * devices + 1 - N_PATCH)
    base_count = capacity // 2 + capacity // 2 * distance * distance // ((N_PATCH - 1) * (N_PATCH - 1))
    first_key, second_key = jax.random.split(key)
    removed = jax.random.randint(first_key, (N_PATCH, hop_count), 0, capacity // 16 + 1)
    removed = jnp.where((distance < N_PATCH - 1)[:, None], removed, 0)
    counts = base_count[:, None] - removed
    rows_drawn = jax.random.randint(second_key, (N_PATCH, hop_count, capacity), 0, M_DEV)
    slot_ids = jnp.arange(capacity, dtype=jnp.int32)
    filled = jnp.where(slot_ids[None, None, :] < counts[:, :, None], rows_drawn, M_DEV)
    return filled.astype(jnp.int32).reshape(N_PATCH * hop_count * EB, EDGE_BLOCK)


def draw_neighbours(key, part):
    node_ids = jnp.arange(MESH, dtype=jnp.int32)
    owners = node_ids // M_DEV
    first_key, second_key = jax.random.split(key)
    steps_drawn = jax.random.randint(first_key, (MESH, KNB), -REACH, REACH + 1)
    rows_drawn = jax.random.randint(second_key, (MESH, KNB), 0, M_DEV)
    others = (owners[:, None] + steps_drawn) % N_PATCH * M_DEV + rows_drawn
    leading = jnp.arange(KNB, dtype=jnp.int32)[None, :] == 0
    return jnp.where(leading, node_ids[:, None], others).astype(jnp.int32)


def place_ends(drawn, rng, smallest, high):
    spot = [jax.random.randint(jax.random.fold_in(rng, axis), (), 0, length) for axis, length in enumerate(drawn.shape)]
    main_axis = drawn.shape.index(max(drawn.shape))
    next_to = spot[:main_axis] + [(spot[main_axis] + 1) % drawn.shape[main_axis]] + spot[main_axis + 1:]
    return drawn.at[tuple(spot)].set(smallest).at[tuple(next_to)].set(high)


def block_scale(own_key, dims, cuts, smallest, high):
    level = 1.0
    for axis_at, parts in cuts:
        draws = jax.random.uniform(jax.random.fold_in(jax.random.fold_in(own_key, 6), axis_at), (parts,), jnp.float32, smallest / len(cuts), high / len(cuts))
        level = level * jnp.repeat(jnp.exp(draws), dims[axis_at] // parts).reshape((-1,) + (1,) * (len(dims) - 1 - axis_at))
    return level


def bell_draw(stream_key, dims, scale, most, shards=(), held_as=jnp.bfloat16):
    values = scale * jax.random.normal(stream_key, dims, jnp.float32)
    if shards:
        values = values * block_scale(stream_key, dims, shards, -0.22, 0.18)
    return jnp.clip(values, -most, most).astype(held_as)


def setup_inputs(seed: int = 0, part: int = 0) -> dict:
    streams_of = jax.random.split(jax.random.key(seed), 21)
    part_keys = jax.random.split(jax.random.fold_in(streams_of[20], part), 21)
    grid_latents = bell_draw(part_keys[0], (GRID, D), 1.0, 6.0, ((0, 16),))
    mesh_latents = bell_draw(part_keys[1], (MESH, D), 1.0, 6.0, ((0, 16),))
    enc_send = place_ends(jax.random.randint(part_keys[2], (BLOCKS, EDGE_BLOCK), 0, G_DEV), jax.random.fold_in(part_keys[2], 1), 0, G_DEV - 1).astype(jnp.int32)
    enc_recv = draw_enc_recv(jax.random.fold_in(jax.random.fold_in(streams_of[20], part), 71), part)
    neighbours = draw_neighbours(jax.random.fold_in(jax.random.fold_in(streams_of[20], part), 71), part)
    enc_grid_w = bell_draw(streams_of[5], (D, D), D ** -0.5, 0.25)
    enc_bias = bell_draw(streams_of[6], (D,), 1.0, 4.0, (), jnp.float32)
    enc_mesh_w = bell_draw(streams_of[7], (D, D), D ** -0.5, 0.25)
    enc_msg_w = bell_draw(streams_of[8], (D, D), D ** -0.5, 0.25)
    upd_agg_w = bell_draw(streams_of[9], (D, D), D ** -0.5, 0.25)
    upd_mesh_w = bell_draw(streams_of[10], (D, D), D ** -0.5, 0.25)
    upd_out_w = bell_draw(streams_of[11], (D, D), D ** -0.5, 0.25)
    norm_gain = jnp.clip(1.0 + 0.18 * jax.random.normal(streams_of[12], (D,), jnp.float32), 0.1, 1.9)
    query_w = bell_draw(streams_of[13], (D, D), D ** -0.5, 0.25)
    key_w = bell_draw(streams_of[14], (D, D), D ** -0.5, 0.25)
    value_w = bell_draw(streams_of[15], (D, D), D ** -0.5, 0.25)
    out_w = bell_draw(streams_of[16], (D, D), D ** -0.5, 0.25)
    ffn_gain = jnp.clip(1.0 + 0.18 * jax.random.normal(streams_of[17], (D,), jnp.float32), 0.1, 1.9)
    ffn_in_w = bell_draw(streams_of[18], (D, FF), D ** -0.5, 0.25)
    ffn_out_w = bell_draw(streams_of[19], (FF, D), FF ** -0.5, 0.125)
    return {"grid_latents": grid_latents, "mesh_latents": mesh_latents, "enc_send": enc_send, "enc_recv": enc_recv, "neighbours": neighbours, "enc_grid_w": enc_grid_w, "enc_bias": enc_bias, "enc_mesh_w": enc_mesh_w, "enc_msg_w": enc_msg_w, "upd_agg_w": upd_agg_w, "upd_mesh_w": upd_mesh_w, "upd_out_w": upd_out_w, "norm_gain": norm_gain, "query_w": query_w, "key_w": key_w, "value_w": value_w, "out_w": out_w, "ffn_gain": ffn_gain, "ffn_in_w": ffn_in_w, "ffn_out_w": ffn_out_w}


norm_eps = 1e-05
head_eps = 1e-06

def rms_scale(values, gain_vector):
    square = lax.optimization_barrier(jnp.mean(values * values, axis=-1, keepdims=True))
    return (values * lax.rsqrt(square + norm_eps) * gain_vector).astype(jnp.bfloat16)

def reference(grid_latents, mesh_latents, enc_send, enc_recv, neighbours, enc_grid_w, enc_bias, enc_mesh_w, enc_msg_w, upd_agg_w, upd_mesh_w, upd_out_w, norm_gain, query_w, key_w, value_w, out_w, ffn_gain, ffn_in_w, ffn_out_w):
    hop_count = 2 * REACH + 1
    capacity = EB * EDGE_BLOCK
    projected = (jnp.dot(grid_latents, enc_grid_w, preferred_element_type=jnp.float32) + enc_bias).astype(jnp.bfloat16)
    receiver_proj = jnp.dot(mesh_latents, enc_mesh_w, preferred_element_type=jnp.float32).astype(jnp.bfloat16)
    senders = enc_send.reshape(N_PATCH, hop_count, capacity)
    targets = enc_recv.reshape(N_PATCH, hop_count, capacity)
    devices = jnp.arange(N_PATCH, dtype=jnp.int32)[:, None, None]
    offsets = (jnp.arange(hop_count, dtype=jnp.int32) - REACH)[None, :, None]
    owners = (devices + offsets) % N_PATCH
    sender_ids = (devices * G_DEV + senders).reshape(N_PATCH, -1)
    receiver_ids = (owners * M_DEV + jnp.minimum(targets, M_DEV - 1)).reshape(N_PATCH, -1)
    segment_ids = jnp.where(targets < M_DEV, owners * M_DEV + targets, MESH).astype(jnp.int32).reshape(N_PATCH, -1)

    def add_device(summed, inputs):
        send_rows = jnp.take(projected, inputs[0], axis=0).astype(jnp.float32)
        recv_rows = jnp.take(receiver_proj, inputs[1], axis=0).astype(jnp.float32)
        active = jax.nn.silu(send_rows + recv_rows).astype(jnp.bfloat16)
        message = jnp.dot(active, enc_msg_w, preferred_element_type=jnp.float32).astype(jnp.bfloat16)
        return (summed + jax.ops.segment_sum(message.astype(jnp.float32), inputs[2], num_segments=MESH + 1), None)
    summed, _ = lax.scan(add_device, jnp.zeros((MESH + 1, D), jnp.float32), (sender_ids, receiver_ids, segment_ids))
    aggregate = summed[:MESH].astype(jnp.bfloat16)
    update = jax.nn.silu(jnp.dot(aggregate, upd_agg_w, preferred_element_type=jnp.float32) + jnp.dot(mesh_latents, upd_mesh_w, preferred_element_type=jnp.float32)).astype(jnp.bfloat16)
    encoded = mesh_latents.astype(jnp.float32) + jnp.dot(update, upd_out_w, preferred_element_type=jnp.float32)
    normed = rms_scale(encoded, norm_gain)
    queries = jnp.dot(normed, query_w, preferred_element_type=jnp.float32).astype(jnp.bfloat16)
    key_proj = jnp.dot(normed, key_w, preferred_element_type=jnp.float32).astype(jnp.bfloat16)
    values = jnp.dot(normed, value_w, preferred_element_type=jnp.float32).astype(jnp.bfloat16)
    head_size = D // HEADS

    def attend(inputs):
        block_queries, block_links = inputs
        row_count = block_queries.shape[0]
        neighbour_key_rows = jnp.take(key_proj, block_links.reshape(-1), axis=0).astype(jnp.float32).reshape(row_count, KNB, HEADS, head_size)
        neighbour_value_rows = jnp.take(values, block_links.reshape(-1), axis=0).astype(jnp.float32).reshape(row_count, KNB, HEADS, head_size)
        query_per_head = block_queries.astype(jnp.float32).reshape(row_count, HEADS, head_size)
        score_products = jnp.einsum('jou,jsou->jso', query_per_head, neighbour_key_rows)
        query_squares = jnp.einsum('tfe,tfe->tf', query_per_head, query_per_head)
        key_sq = jnp.einsum('mkhd,mkhd->mkh', neighbour_key_rows, neighbour_key_rows)
        scores = score_products * lax.rsqrt(query_squares / head_size + head_eps)[:, None, :] * lax.rsqrt(key_sq / head_size + head_eps) / math.sqrt(head_size)
        exponent = jnp.exp(scores)
        attention_weights = (exponent / lax.optimization_barrier(jnp.sum(exponent, axis=1, keepdims=True))).astype(jnp.bfloat16)
        attention_mixture = jnp.einsum('oia,oiae->oae', attention_weights.astype(jnp.float32), neighbour_value_rows)
        return attention_mixture.astype(jnp.bfloat16).reshape(row_count, D)
    attended = lax.map(attend, (queries.reshape(N_PATCH, M_DEV, D), neighbours.reshape(N_PATCH, M_DEV, KNB))).reshape(MESH, D)
    hidden = encoded + jnp.dot(attended, out_w, preferred_element_type=jnp.float32)
    normed_ffn = rms_scale(hidden, ffn_gain)
    expanded = jax.nn.silu(jnp.dot(normed_ffn, ffn_in_w, preferred_element_type=jnp.float32)).astype(jnp.bfloat16)
    return (hidden + jnp.dot(expanded, ffn_out_w, preferred_element_type=jnp.float32)).astype(jnp.bfloat16)
```

```python
import functools
import math

import jax
import jax.numpy as jnp
from jax import lax
from jax.experimental import pallas as pl
from jax.experimental.pallas import tpu as pltpu
from jax.sharding import PartitionSpec as P

HEADS = 4
REACH = 2
LANES = 128
SUBLANES = 8

norm_eps = 1e-05
head_eps = 1e-06


f32 = jnp.float32
bf16 = jnp.bfloat16


def shifted(block, axis, distance):
    devices = range(lax.axis_size(axis))
    route = [((i - distance) % len(devices), i) for i in devices]
    return lax.ppermute(block, axis, route)


def mm(a, b):
    return jnp.dot(a, b, preferred_element_type=f32)


def silu(x):
    half = 0.5 * x
    return half + half * jnp.tanh(half)


def rms_scale(values, gain_vector):
    square = jnp.mean(values * values, axis=-1, keepdims=True)
    return (values * lax.rsqrt(square + norm_eps) * gain_vector).astype(bf16)


def onehot_rows(ids, size):
    blocks = []
    for start in range(0, ids.shape[1], LANES):
        across = jnp.broadcast_to(ids[:, start : start + LANES], (LANES, LANES)).T
        lane = lax.broadcasted_iota(jnp.int32, (LANES, LANES), 1)
        blocks.append(
            jnp.concatenate(
                [
                    jnp.where(across == lane + at, 1.0, 0.0).astype(bf16)
                    for at in range(0, size, LANES)
                ],
                axis=1,
            )
        )
    return jnp.concatenate(blocks, axis=0)


def onehot_columns(ids, size):
    row = lax.broadcasted_iota(jnp.int32, (size, ids.shape[1]), 0)
    return jnp.where(row == ids, 1.0, 0.0).astype(bf16)


def project_kernel(slots, grid_ref, w_ref, bias_ref, send_ref, projected_ref, *outs):
    projected_ref[...] = (mm(grid_ref[...], w_ref[...]) + bias_ref[...]).astype(bf16)
    pick_kernel(slots, projected_ref, send_ref, *outs)


def pick_kernel(slots, projected_ref, send_ref, *outs):
    for slot, out in zip(slots, outs):
        chosen = onehot_rows(send_ref[slot : slot + 1, :], projected_ref.shape[0])
        out[...] = mm(chosen, projected_ref[...]).astype(bf16)


def edge_sum(send_rows, landing, receiver_proj, msg_w):
    size = receiver_proj.shape[0]
    recv_rows = mm(onehot_rows(landing, size), receiver_proj)
    active = silu(send_rows.astype(f32) + recv_rows).astype(bf16)
    message = mm(active, msg_w).astype(bf16)
    return mm(onehot_columns(landing, size), message)


def own_edges_kernel(
    slot, mesh_ref, mesh_w_ref, projected_ref, send_ref, land_ref, msg_w_ref, proj_ref, sum_ref
):
    proj_ref[...] = mm(mesh_ref[...], mesh_w_ref[...]).astype(bf16)
    chosen = onehot_rows(send_ref[slot : slot + 1, :], projected_ref.shape[0])
    rows = mm(chosen, projected_ref[...]).astype(bf16)
    sum_ref[...] = edge_sum(rows, land_ref[slot : slot + 1, :], proj_ref[...], msg_w_ref[...])


def edges_kernel(a_ref, b_ref, la_ref, lb_ref, proj_ref, msg_w_ref, sum_ref, out_ref):
    out_ref[...] = sum_ref[...] + edge_sum(a_ref[...], la_ref[...], proj_ref[...], msg_w_ref[...])
    out_ref[...] += edge_sum(b_ref[...], lb_ref[...], proj_ref[...], msg_w_ref[...])


def update_kernel(
    a_ref, b_ref, la_ref, lb_ref, proj_ref, msg_w_ref, sum_ref,
    mesh_ref, agg_w_ref, mesh_w_ref, out_w_ref, gain_ref,
    encoded_ref, normed_ref,
):
    summed = sum_ref[...] + edge_sum(a_ref[...], la_ref[...], proj_ref[...], msg_w_ref[...])
    summed += edge_sum(b_ref[...], lb_ref[...], proj_ref[...], msg_w_ref[...])
    update = silu(
        mm(summed.astype(bf16), agg_w_ref[...]) + mm(mesh_ref[...], mesh_w_ref[...])
    ).astype(bf16)
    encoded = mesh_ref[...].astype(f32) + mm(update, out_w_ref[...])
    encoded_ref[...] = encoded
    normed_ref[...] = rms_scale(encoded, gain_ref[...])


def count_kernel(width, per_row, pos_ref, out_ref):
    tiles = width // LANES
    depth = pos_ref.shape[1]

    def eight(row):
        ids = pos_ref[pl.ds(row, 1), :]
        node = lax.broadcasted_iota(jnp.int32, (1, depth), 1) // per_row
        high = (ids // LANES) * SUBLANES + node
        left = onehot_columns(high, tiles * SUBLANES)
        right = onehot_columns(ids % LANES, LANES)
        return lax.dot_general(
            left, right, (((1,), (1,)), ((), ())), preferred_element_type=f32
        )

    def step(i, carry):
        first = eight(2 * i)
        second = eight(2 * i + 1)
        for tile in range(tiles):
            rows = slice(tile * SUBLANES, (tile + 1) * SUBLANES)
            both = jnp.concatenate([first[rows], second[rows]], axis=0).astype(bf16)
            out_ref[pl.ds(pl.multiple_of(i * 16, 16), 16), tile * LANES : (tile + 1) * LANES] = both
        return carry

    lax.fori_loop(0, pos_ref.shape[0] // 2, step, 0, unroll=2)


def split_heads(out_ref, wide, normalise, factor):
    head_size = wide.shape[1] // HEADS
    for head in range(HEADS):
        part = wide[:, head * head_size : (head + 1) * head_size]
        if normalise:
            part = part.astype(bf16).astype(f32)
            square = jnp.mean(part * part, axis=-1, keepdims=True)
            part = part * (lax.rsqrt(square + head_eps) * factor)
        out_ref[head] = part.astype(bf16)


def attend_pieces(
    normed_refs, slots, count_ref, key_w_ref, value_w_ref, q_ref, k_buf, v_buf, total_ref, mix_ref, first
):
    rows = k_buf.shape[1]
    for number, (normed_ref, slot) in enumerate(zip(normed_refs, slots)):
        piece = normed_ref[...]
        split_heads(k_buf, mm(piece, key_w_ref[...]), True, 1.0)
        split_heads(v_buf, mm(piece, value_w_ref[...]), False, 1.0)
        fresh = first and number == 0

        def head_step(head, carry):
            scores = lax.dot_general(
                q_ref[head], k_buf[head], (((1,), (1,)), ((), ())), preferred_element_type=f32
            )
            weight = jnp.exp2(scores) * count_ref[:, slot * rows : (slot + 1) * rows].astype(f32)
            partial = weight[:, :LANES]
            for at in range(LANES, rows, LANES):
                partial = partial + weight[:, at : at + LANES]
            mixed = mm(weight.astype(bf16), v_buf[head])
            if fresh:
                total_ref[head] = partial
                mix_ref[head] = mixed
            else:
                total_ref[head] += partial
                mix_ref[head] += mixed
            return carry

        lax.fori_loop(0, HEADS, head_step, 0)


def attend_own_kernel(
    slot, normed_ref, count_ref, query_w_ref, key_w_ref, value_w_ref,
    q_ref, total_ref, mix_ref, k_buf, v_buf,
):
    head_size = k_buf.shape[2]
    factor = math.log2(math.e) / math.sqrt(head_size)
    split_heads(q_ref, mm(normed_ref[...], query_w_ref[...]), True, factor)
    attend_pieces(
        [normed_ref], [slot], count_ref, key_w_ref, value_w_ref, q_ref, k_buf, v_buf, total_ref, mix_ref, True
    )


def attend_more_kernel(
    slots, a_ref, b_ref, count_ref, key_w_ref, value_w_ref, q_ref, total_in, mix_in,
    total_ref, mix_ref, k_buf, v_buf,
):
    total_ref[...] = total_in[...]
    mix_ref[...] = mix_in[...]
    attend_pieces(
        [a_ref, b_ref], slots, count_ref, key_w_ref, value_w_ref, q_ref, k_buf, v_buf, total_ref, mix_ref, False
    )


def finish_kernel(
    slots, a_ref, b_ref, count_ref, key_w_ref, value_w_ref, q_ref, total_in, mix_in,
    encoded_ref, out_w_ref, gain_ref, ffn_in_hbm, ffn_out_hbm,
    result_ref, total_ref, mix_ref, k_buf, v_buf, in_buf, out_buf, sems,
):
    in_copy = pltpu.make_async_copy(ffn_in_hbm, in_buf, sems.at[0])
    out_copy = pltpu.make_async_copy(ffn_out_hbm, out_buf, sems.at[1])
    in_copy.start()
    out_copy.start()
    total_ref[...] = total_in[...]
    mix_ref[...] = mix_in[...]
    attend_pieces(
        [a_ref, b_ref], slots, count_ref, key_w_ref, value_w_ref, q_ref, k_buf, v_buf, total_ref, mix_ref, False
    )
    attended = jnp.concatenate(
        [
            (mix_ref[head] / jnp.sum(total_ref[head], axis=-1, keepdims=True)).astype(bf16)
            for head in range(HEADS)
        ],
        axis=1,
    )
    hidden = encoded_ref[...] + mm(attended, out_w_ref[...])
    normed = rms_scale(hidden, gain_ref[...])
    in_copy.wait()
    out_copy.wait()
    width = in_buf.shape[1]
    chunk = math.gcd(width, 512)
    for at in range(0, width, chunk):
        expanded = silu(mm(normed, in_buf[:, at : at + chunk])).astype(bf16)
        hidden = hidden + mm(expanded, out_buf[at : at + chunk, :])
    result_ref[...] = hidden.astype(bf16)


def call(kernel, name, outs, args, scratch=(), any_args=()):
    vmem = pl.BlockSpec(memory_space=pltpu.VMEM)
    specs = [
        pl.BlockSpec(memory_space=pl.ANY) if i in any_args else vmem for i in range(len(args))
    ]
    shapes = [jax.ShapeDtypeStruct(shape, dtype) for shape, dtype in outs]
    return pl.pallas_call(
        kernel,
        name=name,
        out_shape=shapes,
        in_specs=specs,
        out_specs=[vmem] * len(shapes),
        scratch_shapes=list(scratch),
        compiler_params=pltpu.CompilerParams(vmem_limit_bytes=56 * 1024 * 1024),
    )(*args)


def shards(
    grid_latents,
    mesh_latents,
    enc_send,
    enc_recv,
    neighbours,
    enc_grid_w,
    enc_bias,
    enc_mesh_w,
    enc_msg_w,
    upd_agg_w,
    upd_mesh_w,
    upd_out_w,
    norm_gain,
    query_w,
    key_w,
    value_w,
    out_w,
    ffn_gain,
    ffn_in_w,
    ffn_out_w,
):
    hop_count = 2 * REACH + 1
    rows, width = mesh_latents.shape
    grid_rows = grid_latents.shape[0]
    per_node = neighbours.shape[1]
    head_size = width // HEADS
    senders = enc_send.reshape(hop_count, -1)
    targets = enc_recv.reshape(hop_count, -1)
    capacity = senders.shape[1]
    far = (0, 2 * REACH)
    near = tuple(s for s in range(hop_count) if s not in far and s != REACH)
    piece = ((capacity, width), bf16)

    landing = {
        s: shifted(targets[s : s + 1], "patch", s - REACH) for s in far + near
    }
    projected, *far_rows = call(
        functools.partial(project_kernel, far),
        "project",
        [((grid_rows, width), bf16), piece, piece],
        [grid_latents, enc_grid_w, enc_bias.reshape(1, -1), senders],
    )
    arrived = {s: shifted(r, "patch", s - REACH) for s, r in zip(far, far_rows)}
    near_rows = call(
        functools.partial(pick_kernel, near), "pick", [piece, piece], [projected, senders]
    )
    arrived |= {s: shifted(r, "patch", s - REACH) for s, r in zip(near, near_rows)}
    receiver_proj, summed = call(
        functools.partial(own_edges_kernel, REACH),
        "own_edges",
        [((rows, width), bf16), ((rows, width), f32)],
        [mesh_latents, enc_mesh_w, projected, senders, targets, enc_msg_w],
    )
    own_index = lax.axis_index("patch")
    device_count = lax.axis_size("patch")
    owners = neighbours // rows
    position = (owners - own_index + REACH) % device_count * rows + neighbours % rows
    position = position.reshape(rows // SUBLANES, SUBLANES * per_node)
    (counts,) = call(
        functools.partial(count_kernel, hop_count * rows, per_node),
        "count",
        [((rows, hop_count * rows), bf16)],
        [position],
    )
    (summed,) = call(
        edges_kernel,
        "far_edges",
        [((rows, width), f32)],
        [arrived[far[0]], arrived[far[1]], landing[far[0]], landing[far[1]], receiver_proj, enc_msg_w, summed],
    )
    encoded, normed = call(
        update_kernel,
        "near_update",
        [((rows, width), f32), ((rows, width), bf16)],
        [
            arrived[near[0]], arrived[near[1]], landing[near[0]], landing[near[1]], receiver_proj, enc_msg_w,
            summed, mesh_latents, upd_agg_w, upd_mesh_w, upd_out_w, norm_gain.reshape(1, -1),
        ],
    )
    window = {s: shifted(normed, "patch", REACH - s) for s in far + near}
    by_head = (HEADS, rows, head_size)
    buffers = [pltpu.VMEM(by_head, bf16), pltpu.VMEM(by_head, bf16)]
    totals = ((HEADS, rows, LANES), f32)
    mixes = (by_head, f32)
    queries, total, mix = call(
        functools.partial(attend_own_kernel, REACH),
        "attend_own",
        [(by_head, bf16), totals, mixes],
        [normed, counts, query_w, key_w, value_w],
        buffers,
    )
    total, mix = call(
        functools.partial(attend_more_kernel, near),
        "attend_near",
        [totals, mixes],
        [window[near[0]], window[near[1]], counts, key_w, value_w, queries, total, mix],
        buffers,
    )
    (result,) = call(
        functools.partial(finish_kernel, far),
        "attend_far",
        [((rows, width), bf16)],
        [
            window[far[0]], window[far[1]], counts, key_w, value_w, queries, total, mix,
            encoded, out_w, ffn_gain.reshape(1, -1), ffn_in_w, ffn_out_w,
        ],
        [
            pltpu.VMEM(*totals), pltpu.VMEM(*mixes), *buffers,
            pltpu.VMEM(ffn_in_w.shape, bf16), pltpu.VMEM(ffn_out_w.shape, bf16),
            pltpu.SemaphoreType.DMA((2,)),
        ],
        (11, 12),
    )
    return result


def solution(mesh):
    split = P(("groups", "patch"), None)
    in_specs = (split,) * 5 + (P(),) * 15
    return jax.shard_map(shards, mesh=mesh, in_specs=in_specs, out_specs=split, check_vma=False)
```

```python
import functools
import math

import jax
import jax.numpy as jnp
from jax import lax
from jax.experimental import pallas as pl
from jax.experimental.pallas import tpu as pltpu
from jax.sharding import PartitionSpec as P

HEADS = 4
REACH = 2
LANES = 128
SUBLANES = 8

norm_eps = 1e-05
head_eps = 1e-06


f32 = jnp.float32
bf16 = jnp.bfloat16


def shifted(block, axis, distance):
    devices = range(lax.axis_size(axis))
    route = [((i - distance) % len(devices), i) for i in devices]
    return lax.ppermute(block, axis, route)


def mm(a, b):
    return jnp.dot(a, b, preferred_element_type=f32)


def silu(x):
    half = 0.5 * x
    return half + half * jnp.tanh(half)


def rms_scale(values, gain_vector):
    square = jnp.mean(values * values, axis=-1, keepdims=True)
    return (values * lax.rsqrt(square + norm_eps) * gain_vector).astype(bf16)


def onehot_rows(ids, size):
    blocks = []
    for row in ids:
        across = jnp.broadcast_to(row, (LANES, LANES)).T
        lane = lax.broadcasted_iota(jnp.int32, (LANES, LANES), 1)
        blocks.append(
            jnp.concatenate(
                [
                    jnp.where(across == lane + at, 1.0, 0.0).astype(bf16)
                    for at in range(0, size, LANES)
                ],
                axis=1,
            )
        )
    return jnp.concatenate(blocks, axis=0)


def onehot_columns(ids, size):
    row = lax.broadcasted_iota(jnp.int32, (size, ids.shape[1]), 0)
    return jnp.where(row == ids, 1.0, 0.0).astype(bf16)


def slot_ids(ref, slot, blocks):
    return [ref[slot * blocks + j : slot * blocks + j + 1, :] for j in range(blocks)]


def project_kernel(slots, blocks, grid_ref, w_ref, bias_ref, send_ref, land_ref, projected_ref, *outs):
    projected_ref[...] = (mm(grid_ref[...], w_ref[...]) + bias_ref[...]).astype(bf16)
    pick_kernel(slots, blocks, projected_ref, send_ref, land_ref, *outs)


def pick_kernel(slots, blocks, projected_ref, send_ref, land_ref, *outs):
    capacity = blocks * LANES
    for slot, out in zip(slots, outs):
        chosen = onehot_rows(slot_ids(send_ref, slot, blocks), projected_ref.shape[0])
        out[:capacity, :] = mm(chosen, projected_ref[...]).astype(bf16)
        ids = land_ref[slot * blocks : (slot + 1) * blocks, :]
        parts = jnp.concatenate([(ids // LANES).astype(f32), (ids % LANES).astype(f32)], axis=1)
        spare = jnp.zeros((out.shape[0] - capacity - blocks, 2 * LANES), f32)
        out[capacity:, : 2 * LANES] = jnp.concatenate([parts, spare], axis=0).astype(bf16)
        rest = out.shape[1] - 2 * LANES
        if rest:
            out[capacity:, 2 * LANES :] = jnp.zeros((out.shape[0] - capacity, rest), bf16)


def unpack(ref, blocks):
    capacity = blocks * LANES
    tail = ref[capacity:, : 2 * LANES].astype(f32)
    ids = (tail[:, :LANES] * LANES + tail[:, LANES:]).astype(jnp.int32)
    return ref[:capacity, :], [ids[j : j + 1, :] for j in range(blocks)]


def edge_sum(send_rows, landing, receiver_proj, msg_w):
    size = receiver_proj.shape[0]
    recv_rows = mm(onehot_rows(landing, size), receiver_proj)
    active = silu(send_rows.astype(f32) + recv_rows).astype(bf16)
    message = mm(active, msg_w).astype(bf16)
    return mm(onehot_columns(jnp.concatenate(landing, axis=1), size), message)


def own_edges_kernel(
    slot, blocks, mesh_ref, mesh_w_ref, projected_ref, send_ref, land_ref, msg_w_ref, proj_ref, sum_ref
):
    proj_ref[...] = mm(mesh_ref[...], mesh_w_ref[...]).astype(bf16)
    chosen = onehot_rows(slot_ids(send_ref, slot, blocks), projected_ref.shape[0])
    rows = mm(chosen, projected_ref[...]).astype(bf16)
    sum_ref[...] = edge_sum(rows, slot_ids(land_ref, slot, blocks), proj_ref[...], msg_w_ref[...])


def edges_kernel(blocks, a_ref, b_ref, proj_ref, msg_w_ref, sum_ref, order_ref, out_ref):
    out_ref[...] = sum_ref[...] + edge_sum(*unpack(a_ref, blocks), proj_ref[...], msg_w_ref[...])
    out_ref[...] += edge_sum(*unpack(b_ref, blocks), proj_ref[...], msg_w_ref[...])


def update_kernel(
    blocks, a_ref, b_ref, proj_ref, msg_w_ref, sum_ref,
    mesh_ref, agg_w_ref, mesh_w_ref, out_w_ref, gain_ref,
    encoded_ref, normed_ref,
):
    summed = sum_ref[...] + edge_sum(*unpack(a_ref, blocks), proj_ref[...], msg_w_ref[...])
    summed += edge_sum(*unpack(b_ref, blocks), proj_ref[...], msg_w_ref[...])
    update = silu(
        mm(summed.astype(bf16), agg_w_ref[...]) + mm(mesh_ref[...], mesh_w_ref[...])
    ).astype(bf16)
    encoded = mesh_ref[...].astype(f32) + mm(update, out_w_ref[...])
    encoded_ref[...] = encoded
    normed_ref[...] = rms_scale(encoded, gain_ref[...])


def count_kernel(width, per_row, pos_ref, out_ref):
    tiles = width // LANES
    depth = pos_ref.shape[1]

    def eight(row):
        ids = pos_ref[pl.ds(row, 1), :]
        node = lax.broadcasted_iota(jnp.int32, (1, depth), 1) // per_row
        high = (ids // LANES) * SUBLANES + node
        left = onehot_columns(high, tiles * SUBLANES)
        right = onehot_columns(ids % LANES, LANES)
        return lax.dot_general(
            left, right, (((1,), (1,)), ((), ())), preferred_element_type=f32
        )

    def step(i, carry):
        first = eight(2 * i)
        second = eight(2 * i + 1)
        for tile in range(tiles):
            rows = slice(tile * SUBLANES, (tile + 1) * SUBLANES)
            both = jnp.concatenate([first[rows], second[rows]], axis=0).astype(bf16)
            slot, at = divmod(tile * LANES, out_ref.shape[2])
            out_ref[slot, pl.ds(pl.multiple_of(i * 16, 16), 16), at : at + LANES] = both
        return carry

    lax.fori_loop(0, pos_ref.shape[0] // 2, step, 0, unroll=2)


def split_heads(out_ref, wide, normalise, factor):
    head_size = wide.shape[1] // HEADS
    for head in range(HEADS):
        part = wide[:, head * head_size : (head + 1) * head_size]
        if normalise:
            part = part.astype(bf16).astype(f32)
            square = jnp.mean(part * part, axis=-1, keepdims=True)
            part = part * (lax.rsqrt(square + head_eps) * factor)
        out_ref[head] = part.astype(bf16)


def attend_pieces(
    normed_refs, count_copies, count_buf, key_w_ref, value_w_ref, q_ref, k_buf, v_buf, total_ref, mix_ref, first
):
    rows = k_buf.shape[1]
    for number, normed_ref in enumerate(normed_refs):
        piece = normed_ref[...]
        split_heads(k_buf, mm(piece, key_w_ref[...]), True, 1.0)
        split_heads(v_buf, mm(piece, value_w_ref[...]), False, 1.0)
        fresh = first and number == 0
        count_copies[number].wait()

        def head_step(head, carry):
            scores = lax.dot_general(
                q_ref[head], k_buf[head], (((1,), (1,)), ((), ())), preferred_element_type=f32
            )
            weight = jnp.exp2(scores) * count_buf[number].astype(f32)
            partial = weight[:, :LANES]
            for at in range(LANES, rows, LANES):
                partial = partial + weight[:, at : at + LANES]
            mixed = mm(weight.astype(bf16), v_buf[head])
            if fresh:
                total_ref[head] = partial
                mix_ref[head] = mixed
            else:
                total_ref[head] += partial
                mix_ref[head] += mixed
            return carry

        lax.fori_loop(0, HEADS, head_step, 0)


def start_counts(slots, counts_hbm, count_buf, sems):
    copies = [
        pltpu.make_async_copy(counts_hbm.at[slot], count_buf.at[i], sems.at[i])
        for i, slot in enumerate(slots)
    ]
    for copy in copies:
        copy.start()
    return copies


def attend_close_kernel(
    slot, slots_ref, normed_ref, twin_ref, counts_hbm, query_w_ref, key_w_ref, value_w_ref,
    q_ref, total_ref, mix_ref, passed_ref, k_buf, v_buf, count_buf, sems,
):
    passed_ref[0] = slots_ref[0]
    copies = start_counts([slot, slots_ref[0]], counts_hbm, count_buf, sems)
    head_size = k_buf.shape[2]
    factor = math.log2(math.e) / math.sqrt(head_size)
    split_heads(q_ref, mm(normed_ref[...], query_w_ref[...]), True, factor)
    attend_pieces(
        [normed_ref, twin_ref], copies, count_buf, key_w_ref, value_w_ref, q_ref, k_buf, v_buf, total_ref, mix_ref, True
    )


def attend_far_kernel(
    slots, a_ref, b_ref, counts_hbm, key_w_ref, value_w_ref, q_ref, total_in, mix_in,
    total_ref, mix_ref, k_buf, v_buf, count_buf, sems,
):
    copies = start_counts(slots, counts_hbm, count_buf, sems)
    total_ref[...] = total_in[...]
    mix_ref[...] = mix_in[...]
    attend_pieces(
        [a_ref, b_ref], copies, count_buf, key_w_ref, value_w_ref, q_ref, k_buf, v_buf, total_ref, mix_ref, False
    )


def finish_kernel(
    slots_ref, last_ref, counts_hbm, key_w_ref, value_w_ref, q_ref, total_in, mix_in,
    encoded_ref, out_w_ref, gain_ref, ffn_in_hbm, ffn_out_hbm,
    result_ref, total_ref, mix_ref, in_buf, out_buf, ffn_sems, k_buf, v_buf, count_buf, sems,
):
    copies = start_counts([slots_ref[1]], counts_hbm, count_buf, sems)
    in_copy = pltpu.make_async_copy(ffn_in_hbm, in_buf, ffn_sems.at[0])
    out_copy = pltpu.make_async_copy(ffn_out_hbm, out_buf, ffn_sems.at[1])
    in_copy.start()
    out_copy.start()
    total_ref[...] = total_in[...]
    mix_ref[...] = mix_in[...]
    attend_pieces(
        [last_ref], copies, count_buf, key_w_ref, value_w_ref, q_ref, k_buf, v_buf, total_ref, mix_ref, False
    )
    attended = jnp.concatenate(
        [
            (mix_ref[head] / jnp.sum(total_ref[head], axis=-1, keepdims=True)).astype(bf16)
            for head in range(HEADS)
        ],
        axis=1,
    )
    hidden = encoded_ref[...] + mm(attended, out_w_ref[...])
    normed = rms_scale(hidden, gain_ref[...])
    in_copy.wait()
    out_copy.wait()
    width = in_buf.shape[1]
    chunk = math.gcd(width, 512)
    for at in range(0, width, chunk):
        expanded = silu(mm(normed, in_buf[:, at : at + chunk])).astype(bf16)
        hidden = hidden + mm(expanded, out_buf[at : at + chunk, :])
    result_ref[...] = hidden.astype(bf16)


def call(kernel, name, outs, args, scratch=(), any_args=(), smem_args=(), smem_outs=()):
    vmem = pl.BlockSpec(memory_space=pltpu.VMEM)
    specs = [
        pl.BlockSpec(memory_space=pl.ANY)
        if i in any_args
        else pl.BlockSpec(memory_space=pltpu.SMEM) if i in smem_args else vmem
        for i in range(len(args))
    ]
    shapes = [jax.ShapeDtypeStruct(shape, dtype) for shape, dtype in outs]
    return pl.pallas_call(
        kernel,
        name=name,
        out_shape=shapes,
        in_specs=specs,
        out_specs=[
            pl.BlockSpec(memory_space=pltpu.SMEM) if i in smem_outs else vmem
            for i in range(len(shapes))
        ],
        scratch_shapes=list(scratch),
        compiler_params=pltpu.CompilerParams(vmem_limit_bytes=56 * 1024 * 1024),
    )(*args)


def shards(
    grid_latents,
    mesh_latents,
    enc_send,
    enc_recv,
    neighbours,
    enc_grid_w,
    enc_bias,
    enc_mesh_w,
    enc_msg_w,
    upd_agg_w,
    upd_mesh_w,
    upd_out_w,
    norm_gain,
    query_w,
    key_w,
    value_w,
    out_w,
    ffn_gain,
    ffn_in_w,
    ffn_out_w,
):
    hop_count = 2 * REACH + 1
    rows, width = mesh_latents.shape
    grid_rows = grid_latents.shape[0]
    per_node = neighbours.shape[1]
    head_size = width // HEADS
    blocks = enc_send.shape[0] // hop_count
    far = (0, 2 * REACH)
    near = (REACH - 1, REACH + 1)
    piece = ((blocks * LANES + -(-blocks // 16) * 16, width), bf16)

    projected, *far_rows = call(
        functools.partial(project_kernel, far, blocks),
        "project",
        [((grid_rows, width), bf16), piece, piece],
        [grid_latents, enc_grid_w, enc_bias.reshape(1, -1), enc_send, enc_recv],
    )
    arrived = {s: shifted(r, "patch", s - REACH) for s, r in zip(far, far_rows)}
    near_rows = call(
        functools.partial(pick_kernel, near, blocks),
        "pick",
        [piece, piece],
        [projected, enc_send, enc_recv],
    )
    arrived |= {s: shifted(r, "patch", s - REACH) for s, r in zip(near, near_rows)}
    receiver_proj, summed = call(
        functools.partial(own_edges_kernel, REACH, blocks),
        "own_edges",
        [((rows, width), bf16), ((rows, width), f32)],
        [mesh_latents, enc_mesh_w, projected, enc_send, enc_recv, enc_msg_w],
    )
    own_index = lax.axis_index("patch")
    device_count = lax.axis_size("patch")
    owners = neighbours // rows
    position = (owners - own_index + REACH) % device_count * rows + neighbours % rows
    position = position.reshape(rows // SUBLANES, SUBLANES * per_node)
    (counts,) = call(
        functools.partial(count_kernel, hop_count * rows, per_node),
        "count",
        [((hop_count, rows, rows), bf16)],
        [position],
    )
    (summed,) = call(
        functools.partial(edges_kernel, blocks),
        "far_edges",
        [((rows, width), f32)],
        [arrived[far[0]], arrived[far[1]], receiver_proj, enc_msg_w, summed, counts],
        any_args=(5,),
    )
    encoded, normed = call(
        functools.partial(update_kernel, blocks),
        "near_update",
        [((rows, width), f32), ((rows, width), bf16)],
        [
            arrived[near[0]], arrived[near[1]], receiver_proj, enc_msg_w,
            summed, mesh_latents, upd_agg_w, upd_mesh_w, upd_out_w, norm_gain.reshape(1, -1),
        ],
    )
    swap = [(i, i ^ 1) for i in range(device_count)]
    even = own_index % 2 == 0
    low, high = near
    slots = jnp.where(even, jnp.array([high, low]), jnp.array([low, high])).astype(jnp.int32)
    window = {s: shifted(normed, "patch", REACH - s) for s in far}
    twin = lax.ppermute(normed, "patch", swap)
    by_head = (HEADS, rows, head_size)
    totals = ((HEADS, rows, LANES), f32)
    mixes = (by_head, f32)

    def buffers(pieces):
        return [
            pltpu.VMEM(by_head, bf16),
            pltpu.VMEM(by_head, bf16),
            pltpu.VMEM((pieces, rows, rows), bf16),
            pltpu.SemaphoreType.DMA((pieces,)),
        ]

    queries, total, mix, passed = call(
        functools.partial(attend_close_kernel, REACH),
        "attend_close",
        [(by_head, bf16), totals, mixes, ((1,), jnp.int32)],
        [slots, normed, twin, counts, query_w, key_w, value_w],
        buffers(2),
        (3,),
        (0,),
        (3,),
    )
    onward = jnp.where(passed[0] == high, window[far[1]], window[far[0]])
    last = lax.ppermute(onward, "patch", swap)
    total, mix = call(
        functools.partial(attend_far_kernel, far),
        "attend_far",
        [totals, mixes],
        [window[far[0]], window[far[1]], counts, key_w, value_w, queries, total, mix],
        buffers(2),
        (2,),
    )
    (result,) = call(
        finish_kernel,
        "attend_last",
        [((rows, width), bf16)],
        [
            slots, last, counts, key_w, value_w, queries, total, mix,
            encoded, out_w, ffn_gain.reshape(1, -1), ffn_in_w, ffn_out_w,
        ],
        [
            pltpu.VMEM(*totals), pltpu.VMEM(*mixes),
            pltpu.VMEM(ffn_in_w.shape, bf16), pltpu.VMEM(ffn_out_w.shape, bf16),
            pltpu.SemaphoreType.DMA((2,)), *buffers(1),
        ],
        (2, 11, 12),
        (0,),
    )
    return result


def solution(mesh):
    split = P(("groups", "patch"), None)
    in_specs = (split,) * 5 + (P(),) * 15
    return jax.shard_map(shards, mesh=mesh, in_specs=in_specs, out_specs=split, check_vma=False)
```

```python
import functools
import math

import jax
import jax.numpy as jnp
from jax import lax
from jax.experimental import pallas as pl
from jax.experimental.pallas import tpu as pltpu
from jax.sharding import PartitionSpec as P

HEADS = 4
REACH = 2
LANES = 128
SUBLANES = 8

norm_eps = 1e-05
head_eps = 1e-06


f32 = jnp.float32
bf16 = jnp.bfloat16


def shifted(block, axis, distance):
    devices = range(lax.axis_size(axis))
    route = [((i - distance) % len(devices), i) for i in devices]
    return lax.ppermute(block, axis, route)


def mm(a, b):
    return jnp.dot(a, b, preferred_element_type=f32)


def silu(x):
    half = 0.5 * x
    return half + half * jnp.tanh(half)


def rms_scale(values, gain_vector):
    square = jnp.mean(values * values, axis=-1, keepdims=True)
    return (values * lax.rsqrt(square + norm_eps) * gain_vector).astype(bf16)


def onehot_rows(ids, size):
    blocks = []
    for row in ids:
        across = jnp.broadcast_to(row, (LANES, LANES)).T
        lane = lax.broadcasted_iota(jnp.int32, (LANES, LANES), 1)
        blocks.append(
            jnp.concatenate(
                [
                    jnp.where(across == lane + at, 1.0, 0.0).astype(bf16)
                    for at in range(0, size, LANES)
                ],
                axis=1,
            )
        )
    return jnp.concatenate(blocks, axis=0)


def onehot_columns(ids, size):
    row = lax.broadcasted_iota(jnp.int32, (size, ids.shape[1]), 0)
    return jnp.where(row == ids, 1.0, 0.0).astype(bf16)


def slot_ids(ref, slot, blocks):
    return [ref[slot * blocks + j : slot * blocks + j + 1, :] for j in range(blocks)]


def project_kernel(slots, blocks, grid_ref, w_ref, bias_ref, send_ref, land_ref, projected_ref, *outs):
    projected_ref[...] = (mm(grid_ref[...], w_ref[...]) + bias_ref[...]).astype(bf16)
    pick_kernel(slots, blocks, projected_ref, send_ref, land_ref, *outs)


def pick_kernel(slots, blocks, projected_ref, send_ref, land_ref, *outs):
    capacity = blocks * LANES
    for slot, out in zip(slots, outs):
        chosen = onehot_rows(slot_ids(send_ref, slot, blocks), projected_ref.shape[0])
        out[:capacity, :] = mm(chosen, projected_ref[...]).astype(bf16)
        ids = land_ref[slot * blocks : (slot + 1) * blocks, :]
        parts = jnp.concatenate([(ids // LANES).astype(f32), (ids % LANES).astype(f32)], axis=1)
        spare = jnp.zeros((out.shape[0] - capacity - blocks, 2 * LANES), f32)
        out[capacity:, : 2 * LANES] = jnp.concatenate([parts, spare], axis=0).astype(bf16)
        rest = out.shape[1] - 2 * LANES
        if rest:
            out[capacity:, 2 * LANES :] = jnp.zeros((out.shape[0] - capacity, rest), bf16)


def unpack(ref, blocks):
    capacity = blocks * LANES
    tail = ref[capacity:, : 2 * LANES].astype(f32)
    ids = (tail[:, :LANES] * LANES + tail[:, LANES:]).astype(jnp.int32)
    return ref[:capacity, :], [ids[j : j + 1, :] for j in range(blocks)]


def edge_sum(send_rows, landing, receiver_proj, msg_w):
    size = receiver_proj.shape[0]
    recv_rows = mm(onehot_rows(landing, size), receiver_proj)
    active = silu(send_rows.astype(f32) + recv_rows).astype(bf16)
    message = mm(active, msg_w).astype(bf16)
    return mm(onehot_columns(jnp.concatenate(landing, axis=1), size), message)


def own_edges_kernel(
    slot, blocks, mesh_ref, mesh_w_ref, projected_ref, send_ref, land_ref, msg_w_ref, proj_ref, sum_ref
):
    proj_ref[...] = mm(mesh_ref[...], mesh_w_ref[...]).astype(bf16)
    chosen = onehot_rows(slot_ids(send_ref, slot, blocks), projected_ref.shape[0])
    rows = mm(chosen, projected_ref[...]).astype(bf16)
    sum_ref[...] = edge_sum(rows, slot_ids(land_ref, slot, blocks), proj_ref[...], msg_w_ref[...])


def edges_kernel(blocks, a_ref, b_ref, proj_ref, msg_w_ref, sum_ref, order_ref, out_ref):
    out_ref[...] = sum_ref[...] + edge_sum(*unpack(a_ref, blocks), proj_ref[...], msg_w_ref[...])
    out_ref[...] += edge_sum(*unpack(b_ref, blocks), proj_ref[...], msg_w_ref[...])


def update_kernel(
    blocks, a_ref, b_ref, proj_ref, msg_w_ref, sum_ref,
    mesh_ref, agg_w_ref, mesh_w_ref, out_w_ref, gain_ref,
    encoded_ref, normed_ref, top_ref, bottom_ref,
):
    summed = sum_ref[...] + edge_sum(*unpack(a_ref, blocks), proj_ref[...], msg_w_ref[...])
    summed += edge_sum(*unpack(b_ref, blocks), proj_ref[...], msg_w_ref[...])
    update = silu(
        mm(summed.astype(bf16), agg_w_ref[...]) + mm(mesh_ref[...], mesh_w_ref[...])
    ).astype(bf16)
    encoded = mesh_ref[...].astype(f32) + mm(update, out_w_ref[...])
    encoded_ref[...] = encoded
    normed = rms_scale(encoded, gain_ref[...])
    normed_ref[...] = normed
    half = top_ref.shape[0]
    top_ref[...] = normed[:half]
    bottom_ref[...] = normed[half:]


def count_kernel(width, per_row, pos_ref, out_ref):
    tiles = width // LANES
    depth = pos_ref.shape[1]

    def eight(row):
        ids = pos_ref[pl.ds(row, 1), :]
        node = lax.broadcasted_iota(jnp.int32, (1, depth), 1) // per_row
        high = (ids // LANES) * SUBLANES + node
        left = onehot_columns(high, tiles * SUBLANES)
        right = onehot_columns(ids % LANES, LANES)
        return lax.dot_general(
            left, right, (((1,), (1,)), ((), ())), preferred_element_type=f32
        )

    def step(i, carry):
        first = eight(2 * i)
        second = eight(2 * i + 1)
        for tile in range(tiles):
            rows = slice(tile * SUBLANES, (tile + 1) * SUBLANES)
            both = jnp.concatenate([first[rows], second[rows]], axis=0).astype(bf16)
            slot, at = divmod(tile * LANES, out_ref.shape[2])
            out_ref[slot, pl.ds(pl.multiple_of(i * 16, 16), 16), at : at + LANES] = both
        return carry

    lax.fori_loop(0, pos_ref.shape[0] // 2, step, 0, unroll=2)


def split_heads(out_ref, wide, normalise, factor):
    head_size = wide.shape[1] // HEADS
    for head in range(HEADS):
        part = wide[:, head * head_size : (head + 1) * head_size]
        if normalise:
            part = part.astype(bf16).astype(f32)
            square = jnp.mean(part * part, axis=-1, keepdims=True)
            part = part * (lax.rsqrt(square + head_eps) * factor)
        out_ref[head] = part.astype(bf16)


def attend_pieces(
    normed_refs, count_copies, count_buf, key_w_ref, value_w_ref, q_ref, k_buf, v_buf, total_ref, mix_ref, first
):
    rows = k_buf.shape[1]
    for number, normed_ref in enumerate(normed_refs):
        if isinstance(normed_ref, tuple):
            piece = jnp.concatenate([part[...] for part in normed_ref], axis=0)
        else:
            piece = normed_ref[...]
        split_heads(k_buf, mm(piece, key_w_ref[...]), True, 1.0)
        split_heads(v_buf, mm(piece, value_w_ref[...]), False, 1.0)
        fresh = first and number == 0
        count_copies[number].wait()

        def head_step(head, carry):
            scores = lax.dot_general(
                q_ref[head], k_buf[head], (((1,), (1,)), ((), ())), preferred_element_type=f32
            )
            weight = jnp.exp2(scores) * count_buf[number].astype(f32)
            partial = weight[:, :LANES]
            for at in range(LANES, rows, LANES):
                partial = partial + weight[:, at : at + LANES]
            mixed = mm(weight.astype(bf16), v_buf[head])
            if fresh:
                total_ref[head] = partial
                mix_ref[head] = mixed
            else:
                total_ref[head] += partial
                mix_ref[head] += mixed
            return carry

        lax.fori_loop(0, HEADS, head_step, 0)


def start_counts(slots, counts_hbm, count_buf, sems):
    copies = [
        pltpu.make_async_copy(counts_hbm.at[slot], count_buf.at[i], sems.at[i])
        for i, slot in enumerate(slots)
    ]
    for copy in copies:
        copy.start()
    return copies


def attend_close_kernel(
    slot, slots_ref, normed_ref, twin_ref, counts_hbm, query_w_ref, key_w_ref, value_w_ref,
    q_ref, total_ref, mix_ref, passed_ref, k_buf, v_buf, count_buf, sems,
):
    passed_ref[0] = slots_ref[0]
    copies = start_counts([slot, slots_ref[0]], counts_hbm, count_buf, sems)
    head_size = k_buf.shape[2]
    factor = math.log2(math.e) / math.sqrt(head_size)
    split_heads(q_ref, mm(normed_ref[...], query_w_ref[...]), True, factor)
    attend_pieces(
        [normed_ref, twin_ref], copies, count_buf, key_w_ref, value_w_ref, q_ref, k_buf, v_buf, total_ref, mix_ref, True
    )


def attend_one_kernel(
    which, slots_ref, top_ref, bottom_ref, counts_hbm, key_w_ref, value_w_ref, q_ref, total_in, mix_in,
    total_ref, mix_ref, passed_ref, k_buf, v_buf, count_buf, sems,
):
    passed_ref[0] = slots_ref[0]
    copies = start_counts([slots_ref[which]], counts_hbm, count_buf, sems)
    total_ref[...] = total_in[...]
    mix_ref[...] = mix_in[...]
    attend_pieces(
        [(top_ref, bottom_ref)], copies, count_buf, key_w_ref, value_w_ref, q_ref, k_buf, v_buf, total_ref, mix_ref, False
    )


def finish_kernel(
    slots_ref, last_ref, counts_hbm, key_w_ref, value_w_ref, q_ref, total_in, mix_in,
    encoded_ref, out_w_ref, gain_ref, ffn_in_hbm, ffn_out_hbm,
    result_ref, total_ref, mix_ref, in_buf, out_buf, ffn_sems, k_buf, v_buf, count_buf, sems,
):
    copies = start_counts([slots_ref[1]], counts_hbm, count_buf, sems)
    in_copy = pltpu.make_async_copy(ffn_in_hbm, in_buf, ffn_sems.at[0])
    out_copy = pltpu.make_async_copy(ffn_out_hbm, out_buf, ffn_sems.at[1])
    in_copy.start()
    out_copy.start()
    total_ref[...] = total_in[...]
    mix_ref[...] = mix_in[...]
    attend_pieces(
        [last_ref], copies, count_buf, key_w_ref, value_w_ref, q_ref, k_buf, v_buf, total_ref, mix_ref, False
    )
    attended = jnp.concatenate(
        [
            (mix_ref[head] / jnp.sum(total_ref[head], axis=-1, keepdims=True)).astype(bf16)
            for head in range(HEADS)
        ],
        axis=1,
    )
    hidden = encoded_ref[...] + mm(attended, out_w_ref[...])
    normed = rms_scale(hidden, gain_ref[...])
    in_copy.wait()
    out_copy.wait()
    width = in_buf.shape[1]
    chunk = math.gcd(width, 512)
    for at in range(0, width, chunk):
        expanded = silu(mm(normed, in_buf[:, at : at + chunk])).astype(bf16)
        hidden = hidden + mm(expanded, out_buf[at : at + chunk, :])
    result_ref[...] = hidden.astype(bf16)


def call(kernel, name, outs, args, scratch=(), any_args=(), smem_args=(), smem_outs=()):
    vmem = pl.BlockSpec(memory_space=pltpu.VMEM)
    specs = [
        pl.BlockSpec(memory_space=pl.ANY)
        if i in any_args
        else pl.BlockSpec(memory_space=pltpu.SMEM) if i in smem_args else vmem
        for i in range(len(args))
    ]
    shapes = [jax.ShapeDtypeStruct(shape, dtype) for shape, dtype in outs]
    return pl.pallas_call(
        kernel,
        name=name,
        out_shape=shapes,
        in_specs=specs,
        out_specs=[
            pl.BlockSpec(memory_space=pltpu.SMEM) if i in smem_outs else vmem
            for i in range(len(shapes))
        ],
        scratch_shapes=list(scratch),
        compiler_params=pltpu.CompilerParams(vmem_limit_bytes=56 * 1024 * 1024),
    )(*args)


def shards(
    grid_latents,
    mesh_latents,
    enc_send,
    enc_recv,
    neighbours,
    enc_grid_w,
    enc_bias,
    enc_mesh_w,
    enc_msg_w,
    upd_agg_w,
    upd_mesh_w,
    upd_out_w,
    norm_gain,
    query_w,
    key_w,
    value_w,
    out_w,
    ffn_gain,
    ffn_in_w,
    ffn_out_w,
):
    hop_count = 2 * REACH + 1
    rows, width = mesh_latents.shape
    grid_rows = grid_latents.shape[0]
    per_node = neighbours.shape[1]
    head_size = width // HEADS
    blocks = enc_send.shape[0] // hop_count
    far = (0, 2 * REACH)
    near = (REACH - 1, REACH + 1)
    piece = ((blocks * LANES + -(-blocks // 16) * 16, width), bf16)

    projected, *far_rows = call(
        functools.partial(project_kernel, far, blocks),
        "project",
        [((grid_rows, width), bf16), piece, piece],
        [grid_latents, enc_grid_w, enc_bias.reshape(1, -1), enc_send, enc_recv],
    )
    arrived = {s: shifted(r, "patch", s - REACH) for s, r in zip(far, far_rows)}
    near_rows = call(
        functools.partial(pick_kernel, near, blocks),
        "pick",
        [piece, piece],
        [projected, enc_send, enc_recv],
    )
    arrived |= {s: shifted(r, "patch", s - REACH) for s, r in zip(near, near_rows)}
    receiver_proj, summed = call(
        functools.partial(own_edges_kernel, REACH, blocks),
        "own_edges",
        [((rows, width), bf16), ((rows, width), f32)],
        [mesh_latents, enc_mesh_w, projected, enc_send, enc_recv, enc_msg_w],
    )
    own_index = lax.axis_index("patch")
    device_count = lax.axis_size("patch")
    owners = neighbours // rows
    position = (owners - own_index + REACH) % device_count * rows + neighbours % rows
    position = position.reshape(rows // SUBLANES, SUBLANES * per_node)
    (counts,) = call(
        functools.partial(count_kernel, hop_count * rows, per_node),
        "count",
        [((hop_count, rows, rows), bf16)],
        [position],
    )
    (summed,) = call(
        functools.partial(edges_kernel, blocks),
        "far_edges",
        [((rows, width), f32)],
        [arrived[far[0]], arrived[far[1]], receiver_proj, enc_msg_w, summed, counts],
        any_args=(5,),
    )
    half = ((rows // 2, width), bf16)
    encoded, normed, *halves = call(
        functools.partial(update_kernel, blocks),
        "near_update",
        [((rows, width), f32), ((rows, width), bf16), half, half],
        [
            arrived[near[0]], arrived[near[1]], receiver_proj, enc_msg_w,
            summed, mesh_latents, upd_agg_w, upd_mesh_w, upd_out_w, norm_gain.reshape(1, -1),
        ],
    )
    swap = [(i, i ^ 1) for i in range(device_count)]
    across = [(i, i ^ 2) for i in range(device_count)]
    along = [
        (i, (i + 4 if i // 2 % 2 == 0 else i - 4) % device_count) for i in range(device_count)
    ]
    even = own_index % 2 == 0
    even_pair = own_index // 2 % 2 == 0
    low, high = near
    first, end = far
    slots = jnp.stack(
        [
            jnp.where(even, high, low),
            jnp.where(even, low, high),
            jnp.where(even_pair, end, first),
            jnp.where(even_pair, first, end),
        ]
    ).astype(jnp.int32)
    beside = [lax.ppermute(part, "patch", across) for part in halves]
    twin = lax.ppermute(normed, "patch", swap)
    beyond = [lax.ppermute(beside[0], "patch", along)]
    by_head = (HEADS, rows, head_size)
    totals = ((HEADS, rows, LANES), f32)
    mixes = (by_head, f32)

    def buffers(pieces):
        return [
            pltpu.VMEM(by_head, bf16),
            pltpu.VMEM(by_head, bf16),
            pltpu.VMEM((pieces, rows, rows), bf16),
            pltpu.SemaphoreType.DMA((pieces,)),
        ]

    queries, total, mix, passed = call(
        functools.partial(attend_close_kernel, REACH),
        "attend_close",
        [(by_head, bf16), totals, mixes, ((1,), jnp.int32)],
        [slots, normed, twin, counts, query_w, key_w, value_w],
        buffers(2),
        (3,),
        (0,),
        (3,),
    )
    beside[1] = jnp.where(passed[0] < hop_count, beside[1], jnp.zeros_like(beside[1]))
    beyond.append(lax.ppermute(beside[1], "patch", along))
    total, mix, passed = call(
        functools.partial(attend_one_kernel, 2),
        "attend_beside",
        [totals, mixes, ((1,), jnp.int32)],
        [slots, *beside, counts, key_w, value_w, queries, total, mix],
        buffers(1),
        (3,),
        (0,),
        (2,),
    )
    send_beside = (passed[0] == high) == even_pair
    onward = [jnp.where(send_beside, b, z) for b, z in zip(beside, beyond)]
    last = lax.ppermute(jnp.concatenate(onward, axis=0), "patch", swap)
    total, mix, passed = call(
        functools.partial(attend_one_kernel, 3),
        "attend_beyond",
        [totals, mixes, ((1,), jnp.int32)],
        [slots, *beyond, counts, key_w, value_w, queries, total, mix],
        buffers(1),
        (3,),
        (0,),
        (2,),
    )
    (result,) = call(
        finish_kernel,
        "attend_last",
        [((rows, width), bf16)],
        [
            slots, last, counts, key_w, value_w, queries, total, mix,
            encoded, out_w, ffn_gain.reshape(1, -1), ffn_in_w, ffn_out_w,
        ],
        [
            pltpu.VMEM(*totals), pltpu.VMEM(*mixes),
            pltpu.VMEM(ffn_in_w.shape, bf16), pltpu.VMEM(ffn_out_w.shape, bf16),
            pltpu.SemaphoreType.DMA((2,)), *buffers(1),
        ],
        (2, 11, 12),
        (0,),
    )
    return result


def solution(mesh):
    split = P(("groups", "patch"), None)
    in_specs = (split,) * 5 + (P(),) * 15
    return jax.shard_map(shards, mesh=mesh, in_specs=in_specs, out_specs=split, check_vma=False)
```
